32 devices in a mesh: groups: 2 (over y), bank: 4 (over z), freq: 2 (over x), seg: 2 (over core).
Axes of the slice: x: 2, y: 2, z: 4, core: 2. Of those that a mesh axis runs over, the one named last changes fastest.
Arguments:
- coarse_spectra: bfloat16 [64, 2, 16384], P(('groups', 'seg', 'bank'), None, 'freq'), parts along dimension 0, may hold values from -6 to 6
- fine_spectra: bfloat16 [64, 2, 65536], P(('groups', 'seg', 'bank'), None, 'freq'), parts along dimension 0, may hold values from -6 to 6
- coarse_templates: bfloat16 [2, 2048, 16384], P(None, 'bank', 'freq'), may hold values from -6 to 6
- fine_templates: bfloat16 [2, 4, 64, 65536], P(None, 'bank', None, 'freq'), may hold values from -6 to 6
- coarse_weight: float32 [32768], P(('groups', 'freq')), parts along dimension 0, may hold values from 0.2 to 2
- fine_weight: float32 [131072], P(('groups', 'freq')), parts along dimension 0, may hold values from 0.2 to 2
- triggers: int32 [64, 2], P(('groups', 'seg')), parts along dimension 0, may hold values from 0 to 3, all different within a row; in each aligned block of 4 rows (0 to 3, 4 to 7, ...) at most 2 rows name the same one
- offsets: int32 [64, 2], P(('groups', 'seg')), parts along dimension 0, may hold values from 0 to 131056
Outputs:
- coarse_snr: float32 [2048, 64], P(('bank', 'freq'), ('groups', 'seg')), parts along dimension 1
- fine_snr: float32 [64, 2, 64], P(('groups', 'seg', 'bank'), None, 'freq'), parts along dimension 0
The draws below stay inside these ranges and needn't reach their ends.
There are 2 independent parts, one for each index of `groups`. The reference program is written for one: setup_inputs(seed, part) draws one part's arguments, and reference() takes and returns one part's arrays. A program takes and returns all parts, laid end to end along the dimension named above; an argument that names none is the same for every part. Nothing has to cross between parts.
Inputs may be any that keep to these rules, and one draw needn't show every extreme that they name: `triggers`: each segment names 2 different sub-banks. In each aligned block of 4 segments (the segments of one device along seg and bank) no sub-bank is named more than 2 times.
All inputs are finite; a program needn't handle non-finite values.
Results may differ from the reference program's by a relative error of at most 0.0021.
Values may be sent and summed in bfloat16 or wider, within the bound.
A program may use at most 128 MiB of HBM per device.

```python
import math
import jax
import jax.numpy as jnp
import numpy as np
from jax import lax

FC = 16384
FB = 65536
TC = 2048
TSUB = 64
SEG_DEV = 4
TOP = 2
CAP = 2
LC = 16
LF = 16
CSTRIDE = 2047
SUBBANKS = 4
SEGS = 32


def place_ends(values, rng, smallest, largest):
    spot = [jax.random.randint(jax.random.fold_in(rng, axis), (), 0, length) for axis, length in enumerate(values.shape)]
    main_axis = values.shape.index(max(values.shape))
    beside = spot[:main_axis] + [(spot[main_axis] + 1) % values.shape[main_axis]] + spot[main_axis + 1:]
    return values.at[tuple(spot)].set(smallest).at[tuple(beside)].set(largest)


def block_levels(stream_key, dims, shards, smallest, largest):
    loudness, own = 1.0, jax.random.fold_in(stream_key, 6)
    for position, parts in shards:
        steps = jnp.exp(jax.random.uniform(jax.random.fold_in(own, position), (parts,), jnp.float32, smallest / len(shards), largest / len(shards)))
        loudness = loudness * jnp.repeat(steps, dims[position] // parts).reshape([-1 if axis == position else 1 for axis in range(len(dims))])
    return loudness


def shared_out(stream_key, own, number, rows, count, top, reach, skew):
    ranking = jax.random.permutation(stream_key, count)
    packed, ordinary = portions_of(count, rows * top, reach, skew, True), portions_of(count, rows * top, reach, skew, False)
    places = jnp.arange(count)

    def named(lengths, rotation):
        used = int((lengths > 0).sum())
        fixed = max(1, used // 4)
        passed = fixed + (places - fixed + rotation * (used - fixed)) % max(1, count - fixed)
        return jnp.zeros((count,), jnp.int32).at[ranking[jnp.where(places < fixed, places, passed)]].set(jnp.asarray(lengths, jnp.int32))

    lengths = jnp.where(number % 4 == 0, named(packed, number // 4), named(ordinary, number - number // 4 - 1))
    mixed = jax.random.permutation(jax.random.fold_in(own, 3), count)
    source_of, sink = mixed[0:count // 2 * 2:2], mixed[1:count // 2 * 2:2]
    margin = jnp.minimum(lengths[source_of] - 1, reach - lengths[sink]) // 2
    margin = jnp.where((source_of == ranking[0]) | (sink == ranking[0]) | (lengths[sink] == 0), 0, jnp.maximum(margin, 0))
    passed = jax.random.randint(jax.random.fold_in(own, 4), (count // 2,), 0, 1 << 20) % (margin + 1)
    lengths = lengths.at[source_of].add(-passed).at[sink].add(passed)
    labels = jnp.searchsorted(jnp.cumsum(lengths), jnp.arange(rows * top), side="right").astype(jnp.int32)
    table = labels.reshape(top, rows).T
    table = table[jax.random.permutation(jax.random.fold_in(own, 1), rows)]
    rotation = jax.random.randint(jax.random.fold_in(own, 2), (rows, 1), 0, top)
    return jnp.take_along_axis(table, (jnp.arange(top)[None, :] + rotation) % top, axis=1)


def portions_of(amount, total, bound, skew, full):
    portions = [(1 << 20) // math.isqrt(standing ** skew) + 1 for standing in range(1, amount + 1)]
    largest = bound if full else min(bound, max(-(-total // amount), total * portions[0] // sum(portions)))
    least = 1 if total - largest >= amount - 1 else 0
    given, rest = [largest] + [least] * (amount - 1), total - largest - least * (amount - 1)
    while rest > 0:
        free = [i for i in range(1, amount) if given[i] < largest] or [i for i in range(1, amount) if given[i] < bound]
        pool, left = sum([portions[i] for i in free]), rest
        for i in free:
            addition = min(bound - given[i], max(1, left * portions[i] // pool), rest)
            given[i] = given[i] + addition
            rest = rest - addition
    return np.array(given)


def centred(rng, dims, width, limit, cuts=(), kind=jnp.bfloat16):
    array = width * jax.random.normal(rng, dims, jnp.float32)
    if cuts:
        array = array * block_levels(rng, dims, cuts, -0.22, 0.18)
    return jnp.clip(array, -limit, limit).astype(kind)


def setup_inputs(seed: int = 0, part: int = 0) -> dict:
    key_list = jax.random.split(jax.random.key(seed), 9)
    part_splits = jax.random.split(jax.random.fold_in(key_list[8], part), 9)
    coarse_spectra = centred(part_splits[0], (SEGS, 2, FC), 1.0, 6.0, ((0, 8), (2, 2)))
    fine_spectra = centred(part_splits[1], (SEGS, 2, FB), 1.0, 6.0, ((0, 8), (2, 2)))
    coarse_templates = centred(key_list[2], (2, TC, FC), 1.0, 6.0, ((1, 4), (2, 2)))
    fine_templates = centred(key_list[3], (2, SUBBANKS, TSUB, FB), 1.0, 6.0, ((1, 4), (3, 2)))
    coarse_weight = jnp.clip(jnp.exp(math.log(2.0) - 2.3025851 * jax.random.uniform(part_splits[4], (FC,), jnp.float32) ** block_levels(part_splits[4], (FC,), ((0, 2),), -0.2, 0.2)), 0.2, 2.0)
    fine_weight = jnp.clip(jnp.exp(math.log(2.0) - 2.3025851 * jax.random.uniform(part_splits[5], (FB,), jnp.float32) ** block_levels(part_splits[5], (FB,), ((0, 2),), -0.2, 0.2)), 0.2, 2.0)
    triggers_keys = jax.random.split(jax.random.fold_in(part_splits[6], 1), SEGS // SEG_DEV)
    triggers_turns = jax.random.permutation(jax.random.fold_in(part_splits[6], 3), SEGS // SEG_DEV)
    triggers = jax.vmap(lambda own, number: shared_out(jax.random.fold_in(part_splits[6], 2), own, number, SEG_DEV, SUBBANKS, TOP, CAP, 2))(triggers_keys, triggers_turns).reshape((SEGS, TOP))
    offsets = place_ends(jax.random.randint(part_splits[7], (SEGS, TOP), 0, 2 * FB - LF + 1), jax.random.fold_in(part_splits[7], 1), 0, 2 * FB - LF).astype(jnp.int32)
    return dict(coarse_spectra=coarse_spectra, fine_spectra=fine_spectra, coarse_templates=coarse_templates, fine_templates=fine_templates, coarse_weight=coarse_weight, fine_weight=fine_weight, triggers=triggers, offsets=offsets)


def phase_of(counts, period):
    radians = (2.0 * math.pi / period) * counts.astype(jnp.float32)
    return jnp.cos(radians), jnp.sin(radians)


def offset_count(freq_ids, offset, period):
    upper_bits = offset // 512
    lower_bits = offset % 512
    lower_term = (freq_ids * lower_bits) % period
    upper_term = ((freq_ids * upper_bits) % (period // 512)) * 512
    return (lower_term + upper_term) % period


def lagged(real_part, imag_part, lag_cos, lag_sin):
    left_real = real_part.T[:, :, None]
    left_imag = imag_part.T[:, :, None]
    right_cos = lag_cos[:, None, :]
    right_sin = lag_sin[:, None, :]
    lag_real = (left_real * right_cos - left_imag * right_sin).astype(jnp.bfloat16)
    lag_imag = (left_real * right_sin + left_imag * right_cos).astype(jnp.bfloat16)
    columns = real_part.shape[0] * lag_cos.shape[1]
    return lag_real.reshape(-1, columns), lag_imag.reshape(-1, columns)


def correlate(temp_real, temp_imag, lag_real, lag_imag):
    corr_real = jnp.dot(temp_real, lag_real, preferred_element_type=jnp.float32) + jnp.dot(temp_imag, lag_imag, preferred_element_type=jnp.float32)
    corr_imag = jnp.dot(temp_real, lag_imag, preferred_element_type=jnp.float32) - jnp.dot(temp_imag, lag_real, preferred_element_type=jnp.float32)
    return corr_real, corr_imag


def reference(coarse_spectra, fine_spectra, coarse_templates, fine_templates, coarse_weight, fine_weight, triggers, offsets):
    period_coarse = 2 * FC
    coarse_ids = jnp.arange(FC, dtype=jnp.int32)
    coarse_lags = jnp.arange(LC, dtype=jnp.int32) * CSTRIDE
    coarse_cos, coarse_sin = phase_of((coarse_ids[:, None] * coarse_lags[None, :]) % period_coarse, period_coarse)
    temp_real = coarse_templates[0]
    temp_imag = coarse_templates[1]
    coarse_norm = jnp.sum((temp_real.astype(jnp.float32) ** 2 + temp_imag.astype(jnp.float32) ** 2) * coarse_weight[None, :], axis=1)
    segment_blocks = coarse_spectra.reshape(SEGS // 8, 8, 2, FC)

    def coarse_block(segment_block):
        weighted = segment_block.astype(jnp.float32) * coarse_weight[None, None, :]
        lag_real, lag_imag = lagged(weighted[:, 0], weighted[:, 1], coarse_cos, coarse_sin)
        corr_real, corr_imag = correlate(temp_real, temp_imag, lag_real, lag_imag)
        energy = (corr_real * corr_real + corr_imag * corr_imag).reshape(TC, 8, LC)
        return jnp.max(energy, axis=2)

    peaks = lax.map(coarse_block, segment_blocks)
    coarse_snr = jnp.transpose(peaks, (1, 0, 2)).reshape(TC, SEGS) / coarse_norm[:, None]

    period_fine = 2 * FB
    fine_ids = jnp.arange(FB, dtype=jnp.int32)
    fine_lags = jnp.arange(LF, dtype=jnp.int32)
    fine_cos, fine_sin = phase_of((fine_ids[:, None] * fine_lags[None, :]) % period_fine, period_fine)
    fine_norm = jnp.sum((fine_templates[0].astype(jnp.float32) ** 2 + fine_templates[1].astype(jnp.float32) ** 2) * fine_weight[None, None, :], axis=2)
    pair_segments = jnp.repeat(jnp.arange(SEGS, dtype=jnp.int32), TOP)

    def fine_pair(pair):
        segment_id, bank_id, offset = pair
        spectrum = lax.dynamic_index_in_dim(fine_spectra, segment_id, 0, keepdims=False).astype(jnp.float32) * fine_weight[None, :]
        shift_cos, shift_sin = phase_of(offset_count(fine_ids, offset, period_fine), period_fine)
        shifted_real = spectrum[0] * shift_cos - spectrum[1] * shift_sin
        shifted_imag = spectrum[0] * shift_sin + spectrum[1] * shift_cos
        lag_real, lag_imag = lagged(shifted_real[None, :], shifted_imag[None, :], fine_cos, fine_sin)
        chosen = lax.dynamic_index_in_dim(fine_templates, bank_id, 1, keepdims=False)
        corr_real, corr_imag = correlate(chosen[0], chosen[1], lag_real, lag_imag)
        norm_row = lax.dynamic_index_in_dim(fine_norm, bank_id, 0, keepdims=False)
        return jnp.max(corr_real * corr_real + corr_imag * corr_imag, axis=1) / norm_row

    fine_rows = lax.map(fine_pair, (pair_segments, triggers.reshape(-1).astype(jnp.int32), offsets.reshape(-1).astype(jnp.int32)))
    return coarse_snr, fine_rows.reshape(SEGS, TOP, TSUB)
```

```python
import functools
import math

import jax
import jax.numpy as jnp
import numpy as np
from jax import lax
from jax.experimental import pallas as pl
from jax.experimental.pallas import tpu as pltpu
from jax.sharding import PartitionSpec as P

FC = 16384
FB = 65536
CAP = 2
LC = 16
LF = 16
CSTRIDE = 2047

MESH = pl.DeviceIdType.MESH
F32 = jnp.float32
BF16 = jnp.bfloat16


def phase_of(counts, period):
    radians = 2.0 * math.pi / period * counts.astype(jnp.float32)
    return (jnp.cos(radians), jnp.sin(radians))


def offset_count(freq_ids, offset, period):
    upper_bits = offset // 512
    lower_bits = offset % 512
    lower_term = freq_ids * lower_bits % period
    upper_term = freq_ids * upper_bits % (period // 512) * 512
    return (lower_term + upper_term) % period


def unit_table(count, stride, period):
    angle = 2.0 * np.pi * ((np.arange(count) * stride) % period) / period
    return np.stack([np.cos(angle), np.sin(angle)]).astype(np.float32)


def pair_slots(naming, capacity):
    ranking = jnp.cumsum(naming.astype(jnp.int32), axis=1) - 1
    columns = jnp.arange(capacity, dtype=jnp.int32)
    return naming[:, None, :] & (ranking[:, None, :] == columns[None, :, None])


def nt_dot(left, right):
    return lax.dot_general(left, right, (((1,), (1,)), ((), ())), preferred_element_type=F32)


def lag_rows(real, imag, step_re, step_im, lags):
    reals, imags, pend_re, pend_im = [], [], [], []
    for j in range(lags):
        pend_re.append(real)
        pend_im.append(imag)
        if j % 2 == 1:
            reals.append(jnp.concatenate(pend_re, axis=0).astype(BF16))
            imags.append(jnp.concatenate(pend_im, axis=0).astype(BF16))
            pend_re, pend_im = [], []
        if j + 1 < lags:
            real, imag = real * step_re - imag * step_im, real * step_im + imag * step_re
    return jnp.concatenate(reals, axis=0), jnp.concatenate(imags, axis=0)


def peak(energy, groups, width):
    total = energy.shape[1]
    while total > width:
        half = total // 2
        if half % 128 == 0:
            energy = jnp.maximum(energy[:, :half], energy[:, half:])
        else:
            energy = jnp.maximum(energy, pltpu.roll(energy, energy.shape[1] - half, 1))
        total = half
    return energy[:, :width]


def norm_add(acc, index, rows_of, weight, rows, width):
    group = 32
    for r in range(0, rows, group):
        part = None
        for c in range(0, width, 128):
            hr, hi = rows_of(r, group, c)
            hr = hr.astype(F32)
            hi = hi.astype(F32)
            term = (hr * hr + hi * hi) * weight[:, c : c + 128]
            part = term if part is None else part + term
        acc[index(r), pl.ds(r % acc.shape[1], group), :] += part


def kernel(
    cfg,
    cspec,
    outgoing,
    ctemp,
    ftemp,
    cweight,
    fweight,
    cstep,
    fstep,
    shift_a,
    shift_b,
    csnr,
    fsnr,
    ag,
    slots,
    cacc,
    cnorm,
    facc,
    fsum,
    fnorm,
    crecv,
    cnrecv,
    frecv,
    fnrecv,
    ag_send,
    ag_recv,
    sl_send,
    sl_recv,
    own_sem,
    cx_send,
    cx_recv,
    fx_send,
    fx_recv,
):
    nb, nf, kc, kf, csteps, fsteps, sub = cfg
    step = pl.program_id(0)
    me = lax.axis_index("bank")
    fme = lax.axis_index("freq")
    segs = nb * (cspec.shape[0] // 2)
    seg_dev = cspec.shape[0] // 2
    slot_total = nb * CAP
    crow = cacc.shape[2]
    q = fsum.shape[2]
    nc = segs * LC
    nfl = slot_total * LF

    def ag_copy(d, chunk):
        window = pl.ds(pl.multiple_of(chunk * kc, kc), kc)
        return pltpu.make_async_remote_copy(
            src_ref=cspec.at[:, window],
            dst_ref=ag.at[me, :, window],
            send_sem=ag_send.at[d - 1, chunk],
            recv_sem=ag_recv.at[d - 1, chunk],
            device_id={"bank": lax.rem(me + d, nb)},
            device_id_type=MESH,
        )

    def slot_copy(d, chunk):
        peer = lax.rem(me + d, nb)
        window = pl.ds(pl.multiple_of(chunk * kf, kf), kf)
        return pltpu.make_async_remote_copy(
            src_ref=outgoing.at[peer, :, window],
            dst_ref=slots.at[me, :, window],
            send_sem=sl_send.at[d - 1, chunk],
            recv_sem=sl_recv.at[d - 1, chunk],
            device_id={"bank": peer},
            device_id_type=MESH,
        )

    def own_copies():
        return (
            pltpu.make_async_copy(cspec, ag.at[me], own_sem.at[0]),
            pltpu.make_async_copy(outgoing.at[me], slots.at[me], own_sem.at[1]),
        )

    def freq_copies(pairs, send, recv):
        copies = []
        for d in range(1, nf):
            peer = lax.rem(fme + d, nf)
            for k, (source, target) in enumerate(pairs):
                copies.append(
                    pltpu.make_async_remote_copy(
                        src_ref=source.at[peer],
                        dst_ref=target.at[d - 1],
                        send_sem=send.at[d - 1, k],
                        recv_sem=recv.at[d - 1, k],
                        device_id={"freq": peer},
                        device_id_type=MESH,
                    )
                )
        return copies

    coarse_pairs = ((cacc, crecv), (cnorm, cnrecv))
    fine_pairs = ((fsum, frecv), (fnorm, fnrecv))

    @pl.when(step == 0)
    def _():
        barrier = pltpu.get_barrier_semaphore()
        for d in range(1, nb):
            pl.semaphore_signal(
                barrier, inc=1, device_id={"bank": lax.rem(me + d, nb)}, device_id_type=MESH
            )
        for d in range(1, nf):
            pl.semaphore_signal(
                barrier, inc=1, device_id={"freq": lax.rem(fme + d, nf)}, device_id_type=MESH
            )
        pl.semaphore_wait(barrier, nb - 1 + nf - 1)
        for copy in own_copies():
            copy.start()
        for chunk in range(csteps):
            for d in range(1, nb):
                ag_copy(d, chunk).start()
        cacc[...] = jnp.zeros_like(cacc)
        cnorm[...] = jnp.zeros_like(cnorm)
        facc[...] = jnp.zeros_like(facc)
        fnorm[...] = jnp.zeros_like(fnorm)
        own_copies()[0].wait()

    per = fsteps // csteps

    @pl.when(step < csteps)
    def _():
        for p in range(per):
            for d in range(1, nb):
                slot_copy(d, step * per + p).start()
        for d in range(1, nb):
            ag_copy(d, step).wait_recv()
        weight = cweight[...]
        norm_add(
            cnorm,
            lambda r: r // crow,
            lambda r, n, c: (ctemp[0, r : r + n, c : c + 128], ctemp[1, r : r + n, c : c + 128]),
            weight,
            ctemp.shape[1],
            kc,
        )
        base = step * kc
        for c in range(0, kc, sub):
            window = pl.ds(pl.multiple_of(base + c, sub), sub)
            blocks = [ag[b, :, window].astype(F32) for b in range(nb)]
            w = weight[:, c : c + sub]
            real = jnp.concatenate([x[:seg_dev] for x in blocks], axis=0) * w
            imag = jnp.concatenate([x[seg_dev:] for x in blocks], axis=0) * w
            lag_re, lag_im = lag_rows(
                real, imag, cstep[0:1, c : c + sub], cstep[1:2, c : c + sub], LC
            )
            hr = ctemp[0, :, c : c + sub]
            hi = ctemp[1, :, c : c + sub]
            re = nt_dot(hr, lag_re) + nt_dot(hi, lag_im)
            im = nt_dot(hr, lag_im) + nt_dot(hi, -lag_re)
            for k in range(nf):
                cacc[k, 0] += re[k * crow : (k + 1) * crow]
                cacc[k, 1] += im[k * crow : (k + 1) * crow]

    @pl.when(step >= csteps)
    def _():
        fs = step - csteps

        @pl.when(fs == 0)
        def _():
            own_copies()[1].wait()

        @pl.when(fs == min(1, fsteps - 1))
        def _():
            for copy in freq_copies(coarse_pairs, cx_send, cx_recv):
                copy.start()

        for d in range(1, nb):
            slot_copy(d, fs).wait_recv()
        weight = fweight[...]
        norm_add(
            fnorm,
            lambda r: r // q,
            lambda r, n, c: (
                ftemp[0, 0, r : r + n, c : c + 128],
                ftemp[1, 0, r : r + n, c : c + 128],
            ),
            weight,
            ftemp.shape[2],
            kf,
        ) if q % 32 == 0 else norm_small(fnorm, ftemp, weight, nf, q, kf)
        base = fs * kf
        ar = shift_a[0, 0][:, :1]
        ai = shift_a[1, 0][:, :1]
        for c in range(0, kf, sub):
            window = pl.ds(pl.multiple_of(base + c, sub), sub)
            blocks = [slots[b, :, window].astype(F32) for b in range(nb)]
            w = weight[:, c : c + sub]
            real = jnp.concatenate([x[:CAP] for x in blocks], axis=0) * w
            imag = jnp.concatenate([x[CAP:] for x in blocks], axis=0) * w
            br = shift_b[0, :, c : c + sub]
            bi = shift_b[1, :, c : c + sub]
            sr = ar * br - ai * bi
            si = ar * bi + ai * br
            real, imag = real * sr - imag * si, real * si + imag * sr
            lag_re, lag_im = lag_rows(
                real, imag, fstep[0:1, c : c + sub], fstep[1:2, c : c + sub], LF
            )
            both = jnp.concatenate([lag_re, lag_im], axis=0)
            facc[0] += nt_dot(ftemp[0, 0, :, c : c + sub], both)
            facc[1] += nt_dot(ftemp[1, 0, :, c : c + sub], both)

        @pl.when(fs == fsteps - 1)
        def _():
            re = facc[0, :, :nfl] + facc[1, :, nfl:]
            im = facc[0, :, nfl:] - facc[1, :, :nfl]
            for k in range(nf):
                fsum[k, 0] = re[k * q : (k + 1) * q]
                fsum[k, 1] = im[k * q : (k + 1) * q]
            fcopies = freq_copies(fine_pairs, fx_send, fx_recv)
            for copy in fcopies:
                copy.start()
            ccopies = freq_copies(coarse_pairs, cx_send, cx_recv)
            for copy in ccopies:
                copy.wait_recv()
            re, im, norm = cacc[fme, 0], cacc[fme, 1], cnorm[fme]
            for d in range(nf - 1):
                re = re + crecv[d, 0]
                im = im + crecv[d, 1]
                norm = norm + cnrecv[d]
            top = peak(re * re + im * im, LC, segs)
            csnr[...] = top / jnp.sum(norm, axis=1, keepdims=True)
            for copy in fcopies:
                copy.wait_recv()
            re, im, norm = fsum[fme, 0], fsum[fme, 1], fnorm[fme]
            for d in range(nf - 1):
                re = re + frecv[d, 0]
                im = im + frecv[d, 1]
                norm = norm + fnrecv[d]
            top = peak(re * re + im * im, LF, slot_total)
            fsnr[...] = top / jnp.sum(norm, axis=1, keepdims=True)
            for copy in ccopies + fcopies:
                copy.wait_send()
            for d in range(1, nb):
                for chunk in range(csteps):
                    ag_copy(d, chunk).wait_send()
                for chunk in range(fsteps):
                    slot_copy(d, chunk).wait_send()


def norm_small(acc, ftemp, weight, nf, q, width):
    for k in range(nf):
        part = jnp.zeros((q, 128), F32)
        for c in range(0, width, 128):
            hr = ftemp[0, 0, k * q : (k + 1) * q, c : c + 128].astype(F32)
            hi = ftemp[1, 0, k * q : (k + 1) * q, c : c + 128].astype(F32)
            part = part + (hr * hr + hi * hi) * weight[:, c : c + 128]
        acc[k] += part


def body(
    coarse_spectra,
    fine_spectra,
    coarse_templates,
    fine_templates,
    coarse_weight,
    fine_weight,
    triggers,
    offsets,
):
    nb = lax.axis_size("bank")
    nf = lax.axis_size("freq")
    bank_self = lax.axis_index("bank")
    freq_self = lax.axis_index("freq")
    seg_local = fine_spectra.shape[0]
    cbins = coarse_spectra.shape[2]
    fbins = fine_spectra.shape[2]
    top_count = triggers.shape[1]
    sub_width = fine_templates.shape[2]
    ctemps = coarse_templates.shape[1]
    slot_total = nb * CAP
    segs = nb * seg_local
    kc = min(1024, cbins)
    kf = min(2048, fbins)
    sub = 512
    csteps = cbins // kc
    fsteps = fbins // kf
    crow = ctemps // nf
    q = sub_width // nf

    trig_blocks = triggers.reshape(nb, seg_local * top_count)
    offset_blocks = offsets.reshape(nb, seg_local * top_count)
    recv_pairs = pair_slots(trig_blocks == bank_self, CAP)
    slot_offsets = jnp.sum(jnp.where(recv_pairs, offset_blocks[:, None, :], 0), axis=2).reshape(-1)
    own_pairs = lax.dynamic_index_in_dim(trig_blocks, bank_self, 0, keepdims=False)
    targets = jnp.arange(nb, dtype=jnp.int32)
    send_pairs = pair_slots(own_pairs[None, :] == targets[:, None], CAP)
    send_segments = jnp.any(send_pairs.reshape(nb, CAP, seg_local, top_count), axis=3)
    chooser = (
        send_segments[:, None, :, :, None] & jnp.eye(2, dtype=bool)[None, :, None, None, :]
    ).astype(BF16)
    outgoing = (
        jnp.dot(
            chooser.reshape(nb * 2 * CAP, seg_local * 2),
            fine_spectra.reshape(seg_local * 2, fbins),
            preferred_element_type=F32,
        )
        .astype(BF16)
        .reshape(nb, 2 * CAP, fbins)
    )
    cspec = jnp.transpose(coarse_spectra, (1, 0, 2)).reshape(2 * seg_local, cbins)

    period = 2 * FB
    starts = freq_self * fbins + jnp.arange(fsteps, dtype=jnp.int32) * kf
    shift_a = jnp.stack(
        phase_of(offset_count(starts[:, None], slot_offsets[None, :], period), period)
    )
    shift_a = jnp.broadcast_to(shift_a[:, :, :, None], (2, fsteps, slot_total, 128))
    inner = jnp.arange(kf, dtype=jnp.int32)
    shift_b = jnp.stack(
        phase_of(offset_count(inner[None, :], slot_offsets[:, None], period), period)
    )
    cstep = lax.dynamic_slice_in_dim(
        jnp.asarray(unit_table(FC, CSTRIDE, 2 * FC)), freq_self * cbins, cbins, 1
    )
    fstep = lax.dynamic_slice_in_dim(
        jnp.asarray(unit_table(FB, 1, 2 * FB)), freq_self * fbins, fbins, 1
    )

    nc = segs * LC
    nfl = slot_total * LF

    def cblock(i):
        return jnp.minimum(i, csteps - 1)

    def fblock(i):
        return jnp.maximum(i - csteps, 0)

    whole = pl.BlockSpec(memory_space=pltpu.VMEM)
    dma = pltpu.SemaphoreType.DMA
    csnr, fsnr = pl.pallas_call(
        functools.partial(kernel, (nb, nf, kc, kf, csteps, fsteps, sub)),
        grid=(csteps + fsteps,),
        out_shape=(
            jax.ShapeDtypeStruct((crow, segs), F32),
            jax.ShapeDtypeStruct((q, slot_total), F32),
        ),
        in_specs=[
            whole,
            whole,
            pl.BlockSpec((2, ctemps, kc), lambda i: (0, 0, cblock(i))),
            pl.BlockSpec((2, 1, sub_width, kf), lambda i: (0, 0, 0, fblock(i))),
            pl.BlockSpec((1, kc), lambda i: (0, cblock(i))),
            pl.BlockSpec((1, kf), lambda i: (0, fblock(i))),
            pl.BlockSpec((2, kc), lambda i: (0, cblock(i))),
            pl.BlockSpec((2, kf), lambda i: (0, fblock(i))),
            pl.BlockSpec((2, 1, slot_total, 128), lambda i: (0, fblock(i), 0, 0)),
            whole,
        ],
        out_specs=(whole, whole),
        scratch_shapes=[
            pltpu.VMEM((nb, 2 * seg_local, cbins), BF16),
            pltpu.VMEM((nb, 2 * CAP, fbins), BF16),
            pltpu.VMEM((nf, 2, crow, nc), F32),
            pltpu.VMEM((nf, crow, 128), F32),
            pltpu.VMEM((2, sub_width, 2 * nfl), F32),
            pltpu.VMEM((nf, 2, q, nfl), F32),
            pltpu.VMEM((nf, q, 128), F32),
            pltpu.VMEM((nf - 1, 2, crow, nc), F32),
            pltpu.VMEM((nf - 1, crow, 128), F32),
            pltpu.VMEM((nf - 1, 2, q, nfl), F32),
            pltpu.VMEM((nf - 1, q, 128), F32),
            dma((nb - 1, csteps)),
            dma((nb - 1, csteps)),
            dma((nb - 1, fsteps)),
            dma((nb - 1, fsteps)),
            dma((2,)),
            dma((nf - 1, 2)),
            dma((nf - 1, 2)),
            dma((nf - 1, 2)),
            dma((nf - 1, 2)),
        ],
        compiler_params=pltpu.CompilerParams(
            collective_id=0,
            has_side_effects=True,
            dimension_semantics=("arbitrary",),
            vmem_limit_bytes=60 * 1024 * 1024,
        ),
    )(
        cspec,
        outgoing,
        coarse_templates,
        fine_templates,
        coarse_weight[None, :],
        fine_weight[None, :],
        cstep,
        fstep,
        shift_a,
        shift_b,
    )
    slot_snr = fsnr.T.reshape(nb, CAP, q)
    returned = lax.all_to_all(slot_snr, "bank", split_axis=0, concat_axis=0, tiled=True)
    fine_rows = jnp.sum(
        jnp.where(send_pairs[:, :, :, None], returned[:, :, None, :], 0.0), axis=(0, 1)
    )
    fine_snr = fine_rows.reshape(seg_local, top_count, q)
    return (csnr, fine_snr)


def solution(mesh):
    return jax.shard_map(
        body,
        mesh=mesh,
        in_specs=(
            P(("groups", "seg", "bank"), None, "freq"),
            P(("groups", "seg", "bank"), None, "freq"),
            P(None, "bank", "freq"),
            P(None, "bank", None, "freq"),
            P(("groups", "freq")),
            P(("groups", "freq")),
            P(("groups", "seg"), None),
            P(("groups", "seg"), None),
        ),
        out_specs=(
            P(("bank", "freq"), ("groups", "seg")),
            P(("groups", "seg", "bank"), None, "freq"),
        ),
        check_vma=False,
    )
```

```python
import functools
import math

import jax
import jax.numpy as jnp
import numpy as np
from jax import lax
from jax.experimental import pallas as pl
from jax.experimental.pallas import tpu as pltpu
from jax.sharding import PartitionSpec as P

FC = 16384
FB = 65536
CAP = 2
LC = 16
LF = 16
CSTRIDE = 2047

MESH = pl.DeviceIdType.MESH
F32 = jnp.float32
BF16 = jnp.bfloat16


def phase_of(counts, period):
    radians = 2.0 * math.pi / period * counts.astype(jnp.float32)
    return (jnp.cos(radians), jnp.sin(radians))


def offset_count(freq_ids, offset, period):
    upper_bits = offset // 512
    lower_bits = offset % 512
    lower_term = freq_ids * lower_bits % period
    upper_term = freq_ids * upper_bits % (period // 512) * 512
    return (lower_term + upper_term) % period


def unit_table(count, stride, period):
    angle = 2.0 * np.pi * ((np.arange(count) * stride) % period) / period
    return np.stack([np.cos(angle), np.sin(angle)]).astype(np.float32)


def pair_slots(naming, capacity):
    ranking = jnp.cumsum(naming.astype(jnp.int32), axis=1) - 1
    columns = jnp.arange(capacity, dtype=jnp.int32)
    return naming[:, None, :] & (ranking[:, None, :] == columns[None, :, None])


def nt_dot(left, right):
    return lax.dot_general(left, right, (((1,), (1,)), ((), ())), preferred_element_type=F32)


def lag_rows(real, imag, step_re, step_im, lags):
    reals, imags, pend_re, pend_im = [], [], [], []
    for j in range(lags):
        pend_re.append(real)
        pend_im.append(imag)
        if j % 2 == 1:
            reals.append(jnp.concatenate(pend_re, axis=0).astype(BF16))
            imags.append(jnp.concatenate(pend_im, axis=0).astype(BF16))
            pend_re, pend_im = [], []
        if j + 1 < lags:
            real, imag = real * step_re - imag * step_im, real * step_im + imag * step_re
    return jnp.concatenate(reals, axis=0), jnp.concatenate(imags, axis=0)


def peak(energy, groups, width):
    total = energy.shape[1]
    while total > width:
        half = total // 2
        if half % 128 == 0:
            energy = jnp.maximum(energy[:, :half], energy[:, half:])
        else:
            energy = jnp.maximum(energy, pltpu.roll(energy, energy.shape[1] - half, 1))
        total = half
    return energy


def norm_add(acc, index, rows_of, weight, rows, width):
    group = 32
    for r in range(0, rows, group):
        part = None
        for c in range(0, width, 128):
            hr, hi = rows_of(r, group, c)
            hr = hr.astype(F32)
            hi = hi.astype(F32)
            term = (hr * hr + hi * hi) * weight[:, c : c + 128]
            part = term if part is None else part + term
        acc[index(r), pl.ds(r % acc.shape[1], group), :] += part


def kernel(
    cfg,
    coarse,
    fine,
    chooser,
    giver,
    ctemp,
    ftemp,
    cweight,
    fweight,
    ctable,
    ftable,
    shift_ac,
    shift_as,
    shift_bc,
    shift_bs,
    csnr,
    fout,
    cspec,
    outgoing,
    cstep,
    fstep,
    fsnr,
    back,
    ag,
    slots,
    cacc,
    cnorm,
    facc,
    fsum,
    fnorm,
    crecv,
    cnrecv,
    frecv,
    fnrecv,
    ag_send,
    ag_recv,
    sl_send,
    sl_recv,
    own_sem,
    cx_send,
    cx_recv,
    fx_send,
    fx_recv,
    bk_send,
    bk_recv,
):
    nb, nf, kc, kf, csteps, fsteps, sub = cfg
    step = pl.program_id(0)
    me = lax.axis_index("bank")
    fme = lax.axis_index("freq")
    segs = nb * (cspec.shape[0] // 2)
    seg_dev = cspec.shape[0] // 2
    slot_total = nb * CAP
    crow = cacc.shape[2]
    q = fsum.shape[2]
    nc = segs * LC
    nfl = slot_total * LF

    def ag_copy(d, chunk):
        window = pl.ds(pl.multiple_of(chunk * kc, kc), kc)
        return pltpu.make_async_remote_copy(
            src_ref=cspec.at[:, window],
            dst_ref=ag.at[me, :, window],
            send_sem=ag_send.at[d - 1, chunk],
            recv_sem=ag_recv.at[d - 1, chunk],
            device_id={"bank": lax.rem(me + d, nb)},
            device_id_type=MESH,
        )

    def slot_copy(d, chunk):
        peer = lax.rem(me + d, nb)
        window = pl.ds(pl.multiple_of(chunk * kf, kf), kf)
        return pltpu.make_async_remote_copy(
            src_ref=outgoing.at[peer, :, window],
            dst_ref=slots.at[me, :, window],
            send_sem=sl_send.at[d - 1, chunk],
            recv_sem=sl_recv.at[d - 1, chunk],
            device_id={"bank": peer},
            device_id_type=MESH,
        )

    def table_copies():
        cbins = coarse.shape[2]
        fbins = fine.shape[2]
        return (
            pltpu.make_async_copy(
                ctable.at[:, pl.ds(pl.multiple_of(fme * cbins, cbins), cbins)], cstep, own_sem.at[0]
            ),
            pltpu.make_async_copy(
                ftable.at[:, pl.ds(pl.multiple_of(fme * fbins, fbins), fbins)], fstep, own_sem.at[1]
            ),
        )

    def back_copies():
        return [
            pltpu.make_async_remote_copy(
                src_ref=fsnr,
                dst_ref=back.at[me],
                send_sem=bk_send.at[d - 1],
                recv_sem=bk_recv.at[d - 1],
                device_id={"bank": lax.rem(me + d, nb)},
                device_id_type=MESH,
            )
            for d in range(1, nb)
        ]

    def by_part(block):
        block = block.astype(F32)
        return jnp.concatenate([block[:, 0, :], block[:, 1, :]], axis=0)

    def freq_copies(pairs, send, recv):
        copies = []
        for d in range(1, nf):
            peer = lax.rem(fme + d, nf)
            for k, (source, target) in enumerate(pairs):
                copies.append(
                    pltpu.make_async_remote_copy(
                        src_ref=source.at[peer],
                        dst_ref=target.at[d - 1],
                        send_sem=send.at[d - 1, k],
                        recv_sem=recv.at[d - 1, k],
                        device_id={"freq": peer},
                        device_id_type=MESH,
                    )
                )
        return copies

    coarse_pairs = ((cacc, crecv), (cnorm, cnrecv))
    fine_pairs = ((fsum, frecv), (fnorm, fnrecv))

    @pl.when(step == 0)
    def _():
        barrier = pltpu.get_barrier_semaphore()
        for d in range(1, nb):
            pl.semaphore_signal(
                barrier, inc=1, device_id={"bank": lax.rem(me + d, nb)}, device_id_type=MESH
            )
        for d in range(1, nf):
            pl.semaphore_signal(
                barrier, inc=1, device_id={"freq": lax.rem(fme + d, nf)}, device_id_type=MESH
            )
        for copy in table_copies():
            copy.start()
        for c in range(0, coarse.shape[2], kc):
            cspec[:, c : c + kc] = by_part(coarse[:, :, c : c + kc]).astype(BF16)
        ag[me] = cspec[...]
        pl.semaphore_wait(barrier, nb - 1 + nf - 1)
        for chunk in range(csteps):
            for d in range(1, nb):
                ag_copy(d, chunk).start()
        cacc[...] = jnp.zeros_like(cacc)
        cnorm[...] = jnp.zeros_like(cnorm)
        facc[...] = jnp.zeros_like(facc)
        fnorm[...] = jnp.zeros_like(fnorm)
        choice = chooser[...]

        @pl.loop(0, fsteps)
        def _(chunk):
            window = pl.ds(pl.multiple_of(chunk * kf, kf), kf)
            parts = by_part(fine[:, :, window]).astype(BF16)
            chosen = jnp.dot(choice, parts, preferred_element_type=F32)
            for b in range(nb):
                outgoing[b, :, window] = chosen[b * 2 * CAP : (b + 1) * 2 * CAP].astype(BF16)

        slots[me] = outgoing[me]
        for copy in table_copies():
            copy.wait()

    per = fsteps // csteps

    @pl.when(step < csteps)
    def _():
        for p in range(per):
            for d in range(1, nb):
                slot_copy(d, step * per + p).start()
        for d in range(1, nb):
            ag_copy(d, step).wait_recv()
        weight = cweight[...]
        norm_add(
            cnorm,
            lambda r: r // crow,
            lambda r, n, c: (ctemp[0, r : r + n, c : c + 128], ctemp[1, r : r + n, c : c + 128]),
            weight,
            ctemp.shape[1],
            kc,
        )
        base = step * kc
        for c in range(0, kc, sub):
            window = pl.ds(pl.multiple_of(base + c, sub), sub)
            blocks = [ag[b, :, window].astype(F32) for b in range(nb)]
            w = weight[:, c : c + sub]
            real = jnp.concatenate([x[:seg_dev] for x in blocks], axis=0) * w
            imag = jnp.concatenate([x[seg_dev:] for x in blocks], axis=0) * w
            lag_re, lag_im = lag_rows(
                real, imag, cstep[0:1, window], cstep[1:2, window], LC
            )
            hr = ctemp[0, :, c : c + sub]
            hi = ctemp[1, :, c : c + sub]
            re = nt_dot(hr, lag_re) + nt_dot(hi, lag_im)
            im = nt_dot(hr, lag_im) + nt_dot(hi, -lag_re)
            for k in range(nf):
                cacc[k, 0] += re[k * crow : (k + 1) * crow]
                cacc[k, 1] += im[k * crow : (k + 1) * crow]

    @pl.when(step >= csteps)
    def _():
        fs = step - csteps

        @pl.when(fs == min(1, fsteps - 1))
        def _():
            for copy in freq_copies(coarse_pairs, cx_send, cx_recv):
                copy.start()

        for d in range(1, nb):
            slot_copy(d, fs).wait_recv()
        weight = fweight[...]
        norm_add(
            fnorm,
            lambda r: r // q,
            lambda r, n, c: (
                ftemp[0, 0, r : r + n, c : c + 128],
                ftemp[1, 0, r : r + n, c : c + 128],
            ),
            weight,
            ftemp.shape[2],
            kf,
        ) if q % 32 == 0 else norm_small(fnorm, ftemp, weight, nf, q, kf)
        base = fs * kf
        here = lax.broadcasted_iota(jnp.int32, shift_ac.shape, 1) == fs
        ar = jnp.sum(jnp.where(here, shift_ac[...], 0.0), axis=1, keepdims=True)
        ai = jnp.sum(jnp.where(here, shift_as[...], 0.0), axis=1, keepdims=True)
        for c in range(0, kf, sub):
            window = pl.ds(pl.multiple_of(base + c, sub), sub)
            blocks = [slots[b, :, window].astype(F32) for b in range(nb)]
            w = weight[:, c : c + sub]
            real = jnp.concatenate([x[:CAP] for x in blocks], axis=0) * w
            imag = jnp.concatenate([x[CAP:] for x in blocks], axis=0) * w
            br = shift_bc[:, c : c + sub]
            bi = shift_bs[:, c : c + sub]
            sr = ar * br - ai * bi
            si = ar * bi + ai * br
            real, imag = real * sr - imag * si, real * si + imag * sr
            lag_re, lag_im = lag_rows(
                real, imag, fstep[0:1, window], fstep[1:2, window], LF
            )
            both = jnp.concatenate([lag_re, lag_im], axis=0)
            facc[0] += nt_dot(ftemp[0, 0, :, c : c + sub], both)
            facc[1] += nt_dot(ftemp[1, 0, :, c : c + sub], both)

        @pl.when(fs == fsteps - 1)
        def _():
            re = facc[0, :, :nfl] + facc[1, :, nfl:]
            im = facc[0, :, nfl:] - facc[1, :, :nfl]
            for k in range(nf):
                fsum[k, 0] = re[k * q : (k + 1) * q]
                fsum[k, 1] = im[k * q : (k + 1) * q]
            fcopies = freq_copies(fine_pairs, fx_send, fx_recv)
            for copy in fcopies:
                copy.start()
            ccopies = freq_copies(coarse_pairs, cx_send, cx_recv)
            for copy in ccopies:
                copy.wait_recv()
            re, im, norm = cacc[fme, 0], cacc[fme, 1], cnorm[fme]
            for d in range(nf - 1):
                re = re + crecv[d, 0]
                im = im + crecv[d, 1]
                norm = norm + cnrecv[d]
            top = peak(re * re + im * im, LC, segs)
            csnr[...] = top[:, :segs] / jnp.sum(norm, axis=1, keepdims=True)
            for copy in fcopies:
                copy.wait_recv()
            re, im, norm = fsum[fme, 0], fsum[fme, 1], fnorm[fme]
            for d in range(nf - 1):
                re = re + frecv[d, 0]
                im = im + frecv[d, 1]
                norm = norm + fnrecv[d]
            top = peak(re * re + im * im, LF, slot_total)
            fsnr[...] = top / jnp.sum(norm, axis=1, keepdims=True)
            back[me] = fsnr[...]
            bcopies = back_copies()
            for copy in bcopies:
                copy.start()
            for copy in ccopies + fcopies:
                copy.wait_send()
            for d in range(1, nb):
                for chunk in range(csteps):
                    ag_copy(d, chunk).wait_send()
                for chunk in range(fsteps):
                    slot_copy(d, chunk).wait_send()
            for copy in bcopies:
                copy.wait()
            rows = None
            for b in range(nb):
                part = lax.dot_general(
                    giver[b],
                    back[b],
                    (((1,), (1,)), ((), ())),
                    precision=lax.Precision.HIGHEST,
                    preferred_element_type=F32,
                )
                rows = part if rows is None else rows + part
            fout[...] = rows


def norm_small(acc, ftemp, weight, nf, q, width):
    for k in range(nf):
        part = jnp.zeros((q, 128), F32)
        for c in range(0, width, 128):
            hr = ftemp[0, 0, k * q : (k + 1) * q, c : c + 128].astype(F32)
            hi = ftemp[1, 0, k * q : (k + 1) * q, c : c + 128].astype(F32)
            part = part + (hr * hr + hi * hi) * weight[:, c : c + 128]
        acc[k] += part


def body(
    coarse_spectra,
    fine_spectra,
    coarse_templates,
    fine_templates,
    coarse_weight,
    fine_weight,
    triggers,
    offsets,
):
    nb = lax.axis_size("bank")
    nf = lax.axis_size("freq")
    bank_self = lax.axis_index("bank")
    freq_self = lax.axis_index("freq")
    seg_local = fine_spectra.shape[0]
    cbins = coarse_spectra.shape[2]
    fbins = fine_spectra.shape[2]
    top_count = triggers.shape[1]
    sub_width = fine_templates.shape[2]
    ctemps = coarse_templates.shape[1]
    slot_total = nb * CAP
    segs = nb * seg_local
    kc = min(1024, cbins)
    kf = min(2048, fbins)
    sub = 512
    csteps = cbins // kc
    fsteps = fbins // kf
    crow = ctemps // nf
    q = sub_width // nf

    trig_blocks = triggers.reshape(nb, seg_local * top_count)
    offset_blocks = offsets.reshape(nb, seg_local * top_count)
    recv_pairs = pair_slots(trig_blocks == bank_self, CAP)
    slot_offsets = jnp.sum(jnp.where(recv_pairs, offset_blocks[:, None, :], 0), axis=2).reshape(-1)
    own_pairs = lax.dynamic_index_in_dim(trig_blocks, bank_self, 0, keepdims=False)
    targets = jnp.arange(nb, dtype=jnp.int32)
    send_pairs = pair_slots(own_pairs[None, :] == targets[:, None], CAP)
    send_segments = jnp.any(send_pairs.reshape(nb, CAP, seg_local, top_count), axis=3)
    chooser = (
        send_segments[:, None, :, None, :] & jnp.eye(2, dtype=bool)[None, :, None, :, None]
    ).astype(BF16)
    pairs = seg_local * top_count
    lanes = jnp.arange(128, dtype=jnp.int32) - bank_self * CAP
    giver = sum(
        jnp.where(send_pairs[:, c, :, None] & (lanes == c)[None, None, :], 1.0, 0.0)
        for c in range(CAP)
    )

    period = 2 * FB
    starts = freq_self * fbins + jnp.arange(fsteps, dtype=jnp.int32) * kf
    shift_ac, shift_as = phase_of(
        offset_count(starts[None, :], slot_offsets[:, None], period), period
    )
    inner = jnp.arange(kf, dtype=jnp.int32)
    shift_bc, shift_bs = phase_of(
        offset_count(inner[None, :], slot_offsets[:, None], period), period
    )
    ctable = jnp.asarray(unit_table(FC, CSTRIDE, 2 * FC))
    ftable = jnp.asarray(unit_table(FB, 1, 2 * FB))

    nc = segs * LC
    nfl = slot_total * LF

    def cblock(i):
        return jnp.minimum(i, csteps - 1)

    def fblock(i):
        return jnp.maximum(i - csteps, 0)

    whole = pl.BlockSpec(memory_space=pltpu.VMEM)
    dma = pltpu.SemaphoreType.DMA
    csnr, fine_rows = pl.pallas_call(
        functools.partial(kernel, (nb, nf, kc, kf, csteps, fsteps, sub)),
        grid=(csteps + fsteps,),
        out_shape=(
            jax.ShapeDtypeStruct((crow, segs), F32),
            jax.ShapeDtypeStruct((pairs, q), F32),
        ),
        in_specs=[
            whole,
            whole,
            whole,
            whole,
            pl.BlockSpec((2, ctemps, kc), lambda i: (0, 0, cblock(i))),
            pl.BlockSpec((2, 1, sub_width, kf), lambda i: (0, 0, 0, fblock(i))),
            pl.BlockSpec((1, kc), lambda i: (0, cblock(i))),
            pl.BlockSpec((1, kf), lambda i: (0, fblock(i))),
            pl.BlockSpec(memory_space=pl.ANY),
            pl.BlockSpec(memory_space=pl.ANY),
            whole,
            whole,
            whole,
            whole,
        ],
        out_specs=(whole, whole),
        scratch_shapes=[
            pltpu.VMEM((2 * seg_local, cbins), BF16),
            pltpu.VMEM((nb, 2 * CAP, fbins), BF16),
            pltpu.VMEM((2, cbins), F32),
            pltpu.VMEM((2, fbins), F32),
            pltpu.VMEM((q, 128), F32),
            pltpu.VMEM((nb, q, 128), F32),
            pltpu.VMEM((nb, 2 * seg_local, cbins), BF16),
            pltpu.VMEM((nb, 2 * CAP, fbins), BF16),
            pltpu.VMEM((nf, 2, crow, nc), F32),
            pltpu.VMEM((nf, crow, 128), F32),
            pltpu.VMEM((2, sub_width, 2 * nfl), F32),
            pltpu.VMEM((nf, 2, q, nfl), F32),
            pltpu.VMEM((nf, q, 128), F32),
            pltpu.VMEM((nf - 1, 2, crow, nc), F32),
            pltpu.VMEM((nf - 1, crow, 128), F32),
            pltpu.VMEM((nf - 1, 2, q, nfl), F32),
            pltpu.VMEM((nf - 1, q, 128), F32),
            dma((nb - 1, csteps)),
            dma((nb - 1, csteps)),
            dma((nb - 1, fsteps)),
            dma((nb - 1, fsteps)),
            dma((2,)),
            dma((nf - 1, 2)),
            dma((nf - 1, 2)),
            dma((nf - 1, 2)),
            dma((nf - 1, 2)),
            dma((nb - 1,)),
            dma((nb - 1,)),
        ],
        compiler_params=pltpu.CompilerParams(
            collective_id=0,
            has_side_effects=True,
            dimension_semantics=("arbitrary",),
            vmem_limit_bytes=60 * 1024 * 1024,
        ),
    )(
        coarse_spectra,
        fine_spectra,
        chooser.reshape(nb * 2 * CAP, seg_local * 2),
        giver,
        coarse_templates,
        fine_templates,
        coarse_weight[None, :],
        fine_weight[None, :],
        ctable,
        ftable,
        shift_ac,
        shift_as,
        shift_bc,
        shift_bs,
    )
    fine_snr = fine_rows.reshape(seg_local, top_count, q)
    return (csnr, fine_snr)


def solution(mesh):
    return jax.shard_map(
        body,
        mesh=mesh,
        in_specs=(
            P(("groups", "seg", "bank"), None, "freq"),
            P(("groups", "seg", "bank"), None, "freq"),
            P(None, "bank", "freq"),
            P(None, "bank", None, "freq"),
            P(("groups", "freq")),
            P(("groups", "freq")),
            P(("groups", "seg"), None),
            P(("groups", "seg"), None),
        ),
        out_specs=(
            P(("bank", "freq"), ("groups", "seg")),
            P(("groups", "seg", "bank"), None, "freq"),
        ),
        check_vma=False,
    )
```

```python
import functools
import math

import jax
import jax.numpy as jnp
import numpy as np
from jax import lax
from jax.experimental import pallas as pl
from jax.experimental.pallas import tpu as pltpu
from jax.sharding import PartitionSpec as P

FC = 16384
FB = 65536
CAP = 2
LC = 16
LF = 16
CSTRIDE = 2047

MESH = pl.DeviceIdType.MESH
F32 = jnp.float32
BF16 = jnp.bfloat16


def phase_of(counts, period):
    radians = 2.0 * math.pi / period * counts.astype(jnp.float32)
    return (jnp.cos(radians), jnp.sin(radians))


def offset_count(freq_ids, offset, period):
    upper_bits = offset // 512
    lower_bits = offset % 512
    lower_term = freq_ids * lower_bits % period
    upper_term = freq_ids * upper_bits % (period // 512) * 512
    return (lower_term + upper_term) % period


def unit_table(count, stride, period):
    angle = 2.0 * np.pi * ((np.arange(count) * stride) % period) / period
    return np.stack([np.cos(angle), np.sin(angle)]).astype(np.float32)


def pair_slots(naming, capacity):
    ranking = jnp.cumsum(naming.astype(jnp.int32), axis=1) - 1
    columns = jnp.arange(capacity, dtype=jnp.int32)
    return naming[:, None, :] & (ranking[:, None, :] == columns[None, :, None])


def nt_dot(left, right):
    return lax.dot_general(left, right, (((1,), (1,)), ((), ())), preferred_element_type=F32)


def lag_rows(real, imag, step_re, step_im, lags):
    reals, imags, pend_re, pend_im = [], [], [], []
    for j in range(lags):
        pend_re.append(real)
        pend_im.append(imag)
        if j % 2 == 1:
            reals.append(jnp.concatenate(pend_re, axis=0).astype(BF16))
            imags.append(jnp.concatenate(pend_im, axis=0).astype(BF16))
            pend_re, pend_im = [], []
        if j + 1 < lags:
            real, imag = real * step_re - imag * step_im, real * step_im + imag * step_re
    return jnp.concatenate(reals, axis=0), jnp.concatenate(imags, axis=0)


def peak(energy, groups, width):
    total = energy.shape[1]
    while total > width:
        half = total // 2
        if half % 128 == 0:
            energy = jnp.maximum(energy[:, :half], energy[:, half:])
        else:
            energy = jnp.maximum(energy, pltpu.roll(energy, energy.shape[1] - half, 1))
        total = half
    return energy


def norm_add(acc, index, rows_of, weight, rows, width):
    group = 32
    for r in range(0, rows, group):
        part = None
        for c in range(0, width, 128):
            hr, hi = rows_of(r, group, c)
            hr = hr.astype(F32)
            hi = hi.astype(F32)
            term = (hr * hr + hi * hi) * weight[:, c : c + 128]
            part = term if part is None else part + term
        acc[index(r), pl.ds(r % acc.shape[1], group), :] += part


def kernel(
    cfg,
    coarse,
    fine,
    chooser,
    giver,
    ctemp,
    ftemp,
    cweight,
    fweight,
    ctable,
    ftable,
    shift_ac,
    shift_as,
    shift_bc,
    shift_bs,
    csnr,
    fout,
    cspec,
    outgoing,
    cstep,
    fstep,
    fsnr,
    back,
    ag,
    slots,
    cacc,
    cnorm,
    facc,
    fsum,
    fnorm,
    crecv,
    cnrecv,
    frecv,
    fnrecv,
    ag_send,
    ag_recv,
    sl_send,
    sl_recv,
    own_sem,
    cx_send,
    cx_recv,
    fx_send,
    fx_recv,
    bk_send,
    bk_recv,
):
    nb, nf, kc, kf, csteps, fsteps, sub, fsub = cfg
    step = pl.program_id(0)
    me = lax.axis_index("bank")
    fme = lax.axis_index("freq")
    segs = nb * (cspec.shape[0] // 2)
    seg_dev = cspec.shape[0] // 2
    slot_total = nb * CAP
    crow = cacc.shape[2]
    q = fsum.shape[2]
    nc = segs * LC
    nfl = slot_total * LF

    def ag_copy(d, chunk):
        window = pl.ds(pl.multiple_of(chunk * kc, kc), kc)
        return pltpu.make_async_remote_copy(
            src_ref=cspec.at[:, window],
            dst_ref=ag.at[me, :, window],
            send_sem=ag_send.at[d - 1, chunk],
            recv_sem=ag_recv.at[d - 1, chunk],
            device_id={"bank": lax.rem(me + d, nb)},
            device_id_type=MESH,
        )

    def slot_copy(d, chunk):
        peer = lax.rem(me + d, nb)
        window = pl.ds(pl.multiple_of(chunk * kf, kf), kf)
        return pltpu.make_async_remote_copy(
            src_ref=outgoing.at[peer, :, window],
            dst_ref=slots.at[me, :, window],
            send_sem=sl_send.at[d - 1, chunk],
            recv_sem=sl_recv.at[d - 1, chunk],
            device_id={"bank": peer},
            device_id_type=MESH,
        )

    def table_copies():
        cbins = coarse.shape[2]
        fbins = fine.shape[2]
        return (
            pltpu.make_async_copy(
                ctable.at[:, pl.ds(pl.multiple_of(fme * cbins, cbins), cbins)], cstep, own_sem.at[0]
            ),
            pltpu.make_async_copy(
                ftable.at[:, pl.ds(pl.multiple_of(fme * fbins, fbins), fbins)], fstep, own_sem.at[1]
            ),
        )

    def back_copies():
        return [
            pltpu.make_async_remote_copy(
                src_ref=fsnr,
                dst_ref=back.at[me],
                send_sem=bk_send.at[d - 1],
                recv_sem=bk_recv.at[d - 1],
                device_id={"bank": lax.rem(me + d, nb)},
                device_id_type=MESH,
            )
            for d in range(1, nb)
        ]

    def by_part(block):
        block = block.astype(F32)
        return jnp.concatenate([block[:, 0, :], block[:, 1, :]], axis=0)

    def freq_copies(pairs, send, recv):
        copies = []
        for d in range(1, nf):
            peer = lax.rem(fme + d, nf)
            for k, (source, target) in enumerate(pairs):
                copies.append(
                    pltpu.make_async_remote_copy(
                        src_ref=source.at[peer],
                        dst_ref=target.at[d - 1],
                        send_sem=send.at[d - 1, k],
                        recv_sem=recv.at[d - 1, k],
                        device_id={"freq": peer},
                        device_id_type=MESH,
                    )
                )
        return copies

    coarse_pairs = ((cacc, crecv), (cnorm, cnrecv))
    fine_pairs = ((fsum, frecv), (fnorm, fnrecv))

    @pl.when(step == 0)
    def _():
        barrier = pltpu.get_barrier_semaphore()
        for d in range(1, nb):
            pl.semaphore_signal(
                barrier, inc=1, device_id={"bank": lax.rem(me + d, nb)}, device_id_type=MESH
            )
        for d in range(1, nf):
            pl.semaphore_signal(
                barrier, inc=1, device_id={"freq": lax.rem(fme + d, nf)}, device_id_type=MESH
            )
        for copy in table_copies():
            copy.start()
        for c in range(0, coarse.shape[2], kc):
            cspec[:, c : c + kc] = by_part(coarse[:, :, c : c + kc]).astype(BF16)
        ag[me] = cspec[...]
        pl.semaphore_wait(barrier, nb - 1 + nf - 1)
        for chunk in range(csteps):
            for d in range(1, nb):
                ag_copy(d, chunk).start()
        cacc[...] = jnp.zeros_like(cacc)
        cnorm[...] = jnp.zeros_like(cnorm)
        facc[...] = jnp.zeros_like(facc)
        fnorm[...] = jnp.zeros_like(fnorm)
        choice = chooser[...]

        @pl.loop(0, fsteps)
        def _(chunk):
            window = pl.ds(pl.multiple_of(chunk * kf, kf), kf)
            parts = by_part(fine[:, :, window]).astype(BF16)
            chosen = jnp.dot(choice, parts, preferred_element_type=F32)
            for b in range(nb):
                outgoing[b, :, window] = chosen[b * 2 * CAP : (b + 1) * 2 * CAP].astype(BF16)

        slots[me] = outgoing[me]
        for copy in table_copies():
            copy.wait()

    per = fsteps // csteps

    @pl.when(step < csteps)
    def _():
        for p in range(per):
            for d in range(1, nb):
                slot_copy(d, step * per + p).start()
        for d in range(1, nb):
            ag_copy(d, step).wait_recv()
        weight = cweight[...]
        norm_add(
            cnorm,
            lambda r: r // crow,
            lambda r, n, c: (ctemp[0, r : r + n, c : c + 128], ctemp[1, r : r + n, c : c + 128]),
            weight,
            ctemp.shape[1],
            kc,
        )
        base = step * kc
        for c in range(0, kc, sub):
            window = pl.ds(pl.multiple_of(base + c, sub), sub)
            blocks = [ag[b, :, window].astype(F32) for b in range(nb)]
            w = weight[:, c : c + sub]
            real = jnp.concatenate([x[:seg_dev] for x in blocks], axis=0) * w
            imag = jnp.concatenate([x[seg_dev:] for x in blocks], axis=0) * w
            lag_re, lag_im = lag_rows(
                real, imag, cstep[0:1, window], cstep[1:2, window], LC
            )
            left = jnp.concatenate([ctemp[0, :, c : c + sub], ctemp[1, :, c : c + sub]], axis=1)
            re = nt_dot(left, jnp.concatenate([lag_re, lag_im], axis=1))
            im = nt_dot(left, jnp.concatenate([lag_im, -lag_re], axis=1))
            for k in range(nf):
                cacc[k, 0] += re[k * crow : (k + 1) * crow]
                cacc[k, 1] += im[k * crow : (k + 1) * crow]

    @pl.when(step >= csteps)
    def _():
        fs = step - csteps

        @pl.when(fs == min(1, fsteps - 1))
        def _():
            for copy in freq_copies(coarse_pairs, cx_send, cx_recv):
                copy.start()

        for d in range(1, nb):
            slot_copy(d, fs).wait_recv()
        weight = fweight[...]
        norm_add(
            fnorm,
            lambda r: r // q,
            lambda r, n, c: (
                ftemp[0, 0, r : r + n, c : c + 128],
                ftemp[1, 0, r : r + n, c : c + 128],
            ),
            weight,
            ftemp.shape[2],
            kf,
        ) if q % 32 == 0 else norm_small(fnorm, ftemp, weight, nf, q, kf)
        base = fs * kf
        here = lax.broadcasted_iota(jnp.int32, shift_ac.shape, 1) == fs
        ar = jnp.sum(jnp.where(here, shift_ac[...], 0.0), axis=1, keepdims=True)
        ai = jnp.sum(jnp.where(here, shift_as[...], 0.0), axis=1, keepdims=True)
        for c in range(0, kf, fsub):
            window = pl.ds(pl.multiple_of(base + c, fsub), fsub)
            blocks = [slots[b, :, window].astype(F32) for b in range(nb)]
            w = weight[:, c : c + fsub]
            real = jnp.concatenate([x[:CAP] for x in blocks], axis=0) * w
            imag = jnp.concatenate([x[CAP:] for x in blocks], axis=0) * w
            br = shift_bc[:, c : c + fsub]
            bi = shift_bs[:, c : c + fsub]
            sr = ar * br - ai * bi
            si = ar * bi + ai * br
            real, imag = real * sr - imag * si, real * si + imag * sr
            lag_re, lag_im = lag_rows(
                real, imag, fstep[0:1, window], fstep[1:2, window], LF
            )
            both = jnp.concatenate([lag_re, lag_im], axis=0)
            left = jnp.concatenate(
                [ftemp[0, 0, :, c : c + fsub], ftemp[1, 0, :, c : c + fsub]], axis=0
            )
            facc[...] += nt_dot(left, both)

        @pl.when(fs == fsteps - 1)
        def _():
            half = facc.shape[0] // 2
            re = facc[:half, :nfl] + facc[half:, nfl:]
            im = facc[:half, nfl:] - facc[half:, :nfl]
            for k in range(nf):
                fsum[k, 0] = re[k * q : (k + 1) * q]
                fsum[k, 1] = im[k * q : (k + 1) * q]
            fcopies = freq_copies(fine_pairs, fx_send, fx_recv)
            for copy in fcopies:
                copy.start()
            ccopies = freq_copies(coarse_pairs, cx_send, cx_recv)
            for copy in ccopies:
                copy.wait_recv()
            re, im, norm = cacc[fme, 0], cacc[fme, 1], cnorm[fme]
            for d in range(nf - 1):
                re = re + crecv[d, 0]
                im = im + crecv[d, 1]
                norm = norm + cnrecv[d]
            top = peak(re * re + im * im, LC, segs)
            csnr[...] = top[:, :segs] / jnp.sum(norm, axis=1, keepdims=True)
            for copy in fcopies:
                copy.wait_recv()
            re, im, norm = fsum[fme, 0], fsum[fme, 1], fnorm[fme]
            for d in range(nf - 1):
                re = re + frecv[d, 0]
                im = im + frecv[d, 1]
                norm = norm + fnrecv[d]
            top = peak(re * re + im * im, LF, slot_total)
            fsnr[...] = top / jnp.sum(norm, axis=1, keepdims=True)
            back[me] = fsnr[...]
            bcopies = back_copies()
            for copy in bcopies:
                copy.start()
            for copy in ccopies + fcopies:
                copy.wait_send()
            for d in range(1, nb):
                for chunk in range(csteps):
                    ag_copy(d, chunk).wait_send()
                for chunk in range(fsteps):
                    slot_copy(d, chunk).wait_send()
            for copy in bcopies:
                copy.wait()
            rows = None
            for b in range(nb):
                part = lax.dot_general(
                    giver[b],
                    back[b],
                    (((1,), (1,)), ((), ())),
                    precision=lax.Precision.HIGHEST,
                    preferred_element_type=F32,
                )
                rows = part if rows is None else rows + part
            fout[...] = rows


def norm_small(acc, ftemp, weight, nf, q, width):
    for k in range(nf):
        part = jnp.zeros((q, 128), F32)
        for c in range(0, width, 128):
            hr = ftemp[0, 0, k * q : (k + 1) * q, c : c + 128].astype(F32)
            hi = ftemp[1, 0, k * q : (k + 1) * q, c : c + 128].astype(F32)
            part = part + (hr * hr + hi * hi) * weight[:, c : c + 128]
        acc[k] += part


def body(
    coarse_spectra,
    fine_spectra,
    coarse_templates,
    fine_templates,
    coarse_weight,
    fine_weight,
    triggers,
    offsets,
):
    nb = lax.axis_size("bank")
    nf = lax.axis_size("freq")
    bank_self = lax.axis_index("bank")
    freq_self = lax.axis_index("freq")
    seg_local = fine_spectra.shape[0]
    cbins = coarse_spectra.shape[2]
    fbins = fine_spectra.shape[2]
    top_count = triggers.shape[1]
    sub_width = fine_templates.shape[2]
    ctemps = coarse_templates.shape[1]
    slot_total = nb * CAP
    segs = nb * seg_local
    kc = min(1024, cbins)
    kf = min(2048, fbins)
    sub = 512
    fsub = 1024
    csteps = cbins // kc
    fsteps = fbins // kf
    crow = ctemps // nf
    q = sub_width // nf

    trig_blocks = triggers.reshape(nb, seg_local * top_count)
    offset_blocks = offsets.reshape(nb, seg_local * top_count)
    recv_pairs = pair_slots(trig_blocks == bank_self, CAP)
    slot_offsets = jnp.sum(jnp.where(recv_pairs, offset_blocks[:, None, :], 0), axis=2).reshape(-1)
    own_pairs = lax.dynamic_index_in_dim(trig_blocks, bank_self, 0, keepdims=False)
    targets = jnp.arange(nb, dtype=jnp.int32)
    send_pairs = pair_slots(own_pairs[None, :] == targets[:, None], CAP)
    send_segments = jnp.any(send_pairs.reshape(nb, CAP, seg_local, top_count), axis=3)
    chooser = (
        send_segments[:, None, :, None, :] & jnp.eye(2, dtype=bool)[None, :, None, :, None]
    ).astype(BF16)
    pairs = seg_local * top_count
    lanes = jnp.arange(128, dtype=jnp.int32) - bank_self * CAP
    giver = sum(
        jnp.where(send_pairs[:, c, :, None] & (lanes == c)[None, None, :], 1.0, 0.0)
        for c in range(CAP)
    )

    period = 2 * FB
    starts = freq_self * fbins + jnp.arange(fsteps, dtype=jnp.int32) * kf
    shift_ac, shift_as = phase_of(
        offset_count(starts[None, :], slot_offsets[:, None], period), period
    )
    inner = jnp.arange(kf, dtype=jnp.int32)
    shift_bc, shift_bs = phase_of(
        offset_count(inner[None, :], slot_offsets[:, None], period), period
    )
    ctable = jnp.asarray(unit_table(FC, CSTRIDE, 2 * FC))
    ftable = jnp.asarray(unit_table(FB, 1, 2 * FB))

    nc = segs * LC
    nfl = slot_total * LF

    def cblock(i):
        return jnp.minimum(i, csteps - 1)

    def fblock(i):
        return jnp.maximum(i - csteps, 0)

    whole = pl.BlockSpec(memory_space=pltpu.VMEM)
    dma = pltpu.SemaphoreType.DMA
    csnr, fine_rows = pl.pallas_call(
        functools.partial(kernel, (nb, nf, kc, kf, csteps, fsteps, sub, fsub)),
        grid=(csteps + fsteps,),
        out_shape=(
            jax.ShapeDtypeStruct((crow, segs), F32),
            jax.ShapeDtypeStruct((pairs, q), F32),
        ),
        in_specs=[
            whole,
            whole,
            whole,
            whole,
            pl.BlockSpec((2, ctemps, kc), lambda i: (0, 0, cblock(i))),
            pl.BlockSpec((2, 1, sub_width, kf), lambda i: (0, 0, 0, fblock(i))),
            pl.BlockSpec((1, kc), lambda i: (0, cblock(i))),
            pl.BlockSpec((1, kf), lambda i: (0, fblock(i))),
            pl.BlockSpec(memory_space=pl.ANY),
            pl.BlockSpec(memory_space=pl.ANY),
            whole,
            whole,
            whole,
            whole,
        ],
        out_specs=(whole, whole),
        scratch_shapes=[
            pltpu.VMEM((2 * seg_local, cbins), BF16),
            pltpu.VMEM((nb, 2 * CAP, fbins), BF16),
            pltpu.VMEM((2, cbins), F32),
            pltpu.VMEM((2, fbins), F32),
            pltpu.VMEM((q, 128), F32),
            pltpu.VMEM((nb, q, 128), F32),
            pltpu.VMEM((nb, 2 * seg_local, cbins), BF16),
            pltpu.VMEM((nb, 2 * CAP, fbins), BF16),
            pltpu.VMEM((nf, 2, crow, nc), F32),
            pltpu.VMEM((nf, crow, 128), F32),
            pltpu.VMEM((2 * sub_width, 2 * nfl), F32),
            pltpu.VMEM((nf, 2, q, nfl), F32),
            pltpu.VMEM((nf, q, 128), F32),
            pltpu.VMEM((nf - 1, 2, crow, nc), F32),
            pltpu.VMEM((nf - 1, crow, 128), F32),
            pltpu.VMEM((nf - 1, 2, q, nfl), F32),
            pltpu.VMEM((nf - 1, q, 128), F32),
            dma((nb - 1, csteps)),
            dma((nb - 1, csteps)),
            dma((nb - 1, fsteps)),
            dma((nb - 1, fsteps)),
            dma((2,)),
            dma((nf - 1, 2)),
            dma((nf - 1, 2)),
            dma((nf - 1, 2)),
            dma((nf - 1, 2)),
            dma((nb - 1,)),
            dma((nb - 1,)),
        ],
        compiler_params=pltpu.CompilerParams(
            collective_id=0,
            has_side_effects=True,
            dimension_semantics=("arbitrary",),
            vmem_limit_bytes=60 * 1024 * 1024,
        ),
    )(
        coarse_spectra,
        fine_spectra,
        chooser.reshape(nb * 2 * CAP, seg_local * 2),
        giver,
        coarse_templates,
        fine_templates,
        coarse_weight[None, :],
        fine_weight[None, :],
        ctable,
        ftable,
        shift_ac,
        shift_as,
        shift_bc,
        shift_bs,
    )
    fine_snr = fine_rows.reshape(seg_local, top_count, q)
    return (csnr, fine_snr)


def solution(mesh):
    return jax.shard_map(
        body,
        mesh=mesh,
        in_specs=(
            P(("groups", "seg", "bank"), None, "freq"),
            P(("groups", "seg", "bank"), None, "freq"),
            P(None, "bank", "freq"),
            P(None, "bank", None, "freq"),
            P(("groups", "freq")),
            P(("groups", "freq")),
            P(("groups", "seg"), None),
            P(("groups", "seg"), None),
        ),
        out_specs=(
            P(("bank", "freq"), ("groups", "seg")),
            P(("groups", "seg", "bank"), None, "freq"),
        ),
        check_vma=False,
    )
```
